32 devices in a mesh: tm: 4 (over y, x), space: 8 (over z, core).
Axes of the slice: x: 2, y: 2, z: 4, core: 2. Of those that a mesh axis runs over, the one named last changes fastest.
Arguments:
- fields: bfloat16 [4096, 2, 16384], P('tm', None, 'space')
- calendar_day: int32 [4096], P('tm'), may hold values from 0 to 364, as said below
- events: int32 [16, 96], replicated, may hold values from 0 to 4080, as said below
- lag_offsets: int32 [16], replicated, may hold values from 0 to 15, each once
Outputs:
- composite: float32 [16, 16, 2, 16384], P('tm', None, None, 'space')
The draws below stay inside these ranges and needn't reach their ends.
Inputs may be any that keep to these rules, and one draw needn't show every extreme that they name: `calendar_day`: days of the year of successive record days, one or two calendar days apart. `events`: each entry is a record day; a day may repeat within a type. `lag_offsets`: each of 0 to 15 once.
All inputs are finite; a program needn't handle non-finite values.
Results may differ from the reference program's by a relative error of at most 0.0012.
Values may be sent and summed in bfloat16 or wider, within the bound.
A program may use at most 64 MiB of HBM per device.

```python
import jax
import jax.numpy as jnp
from jax import lax

TYPES = 16
LAGS = 16
MEMBERS = 96
HARMONICS = 4
DAYS = 4096
POINTS = 16384


TWO_PI = 6.283185307179586


def calendar_draw(key):
    day_steps = jax.random.randint(jax.random.fold_in(key, 11), (DAYS,), 1, 3)
    first_day = jax.random.randint(jax.random.fold_in(key, 12), (), 0, 365)
    return jnp.mod(first_day + jnp.cumsum(day_steps), 365).astype(jnp.int32)


def draw_calendar_day(key, part):
    return calendar_draw(key)


def draw_events(key, part):
    early_pick = jax.random.randint(jax.random.fold_in(key, 21), (TYPES, MEMBERS), 0, DAYS - LAGS + 1)
    later_pick = jax.random.randint(jax.random.fold_in(key, 22), (TYPES, MEMBERS), 0, DAYS - LAGS + 1)
    chosen = jnp.minimum(early_pick, later_pick)
    chosen = chosen.at[0, 0].set(DAYS - LAGS).at[1, 0].set(0)
    return chosen.astype(jnp.int32)


def draw_fields(key, part):
    calendar_days = calendar_draw(key)
    phases = calendar_days.astype(jnp.float32) * (TWO_PI / 365.25)
    orders = jnp.arange(1, HARMONICS + 1).astype(jnp.float32)
    angles = phases[:, None] * orders[None, :]
    basis = jnp.concatenate([jnp.cos(angles), jnp.sin(angles)], axis=1)
    subkeys = jax.random.split(jax.random.fold_in(key, 31), 6)
    scaling = jnp.concatenate([orders, orders])
    amplitudes = jax.random.normal(subkeys[0], (2 * HARMONICS, 2 * POINTS), jnp.float32) * 1.5 / scaling[:, None]
    seasonal = jnp.dot(basis, amplitudes, precision=lax.Precision.HIGHEST)
    position = (jnp.arange(2 * POINTS) % POINTS).astype(jnp.float32) / POINTS
    ramp_factor = 1.0 + 2.0 * position
    levels = jax.random.uniform(subkeys[1], (2 * POINTS,), jnp.float32, 0.5, 1.5) * ramp_factor
    offset = jax.random.normal(subkeys[2], (2 * POINTS,), jnp.float32) * 3.0
    fraction = jnp.arange(DAYS).astype(jnp.float32) / DAYS
    noise_part = jax.random.normal(subkeys[3], (DAYS, 2 * POINTS), jnp.float32) * 0.8
    combined = seasonal + offset[None, :] + 2.0 * fraction[:, None] * levels[None, :] + noise_part * ramp_factor[None, :]
    return combined.reshape(DAYS, 2, POINTS).astype(jnp.bfloat16)


def setup_inputs(seed: int = 0) -> dict:
    streams_of = jax.random.split(jax.random.key(seed), 5)
    return {
        "fields": draw_fields(jax.random.fold_in(streams_of[4], 71), 0),
        "calendar_day": draw_calendar_day(jax.random.fold_in(streams_of[4], 71), 0),
        "events": draw_events(jax.random.fold_in(streams_of[4], 71), 0),
        "lag_offsets": jax.random.permutation(streams_of[3], LAGS).astype(jnp.int32),
    }


TWO_PI = 6.283185307179586

def regressors(calendar_day):
    phases = calendar_day.astype(jnp.float32) * (TWO_PI / 365.25)
    columns = [jnp.ones_like(phases)]
    for harmonic in range(1, HARMONICS + 1):
        columns.append(jnp.cos(harmonic * phases))
        columns.append(jnp.sin(harmonic * phases))
    return jnp.stack(columns, axis=1).astype(jnp.bfloat16)

def solve_fit(gram_matrix, projection):
    factor = jnp.linalg.cholesky(gram_matrix)
    return jax.scipy.linalg.cho_solve((factor, True), projection)

def reference(fields, calendar_day, events, lag_offsets):
    design = regressors(calendar_day)
    record = fields.reshape(DAYS, 2 * POINTS)
    gram_matrix = jnp.dot(design.T.astype(jnp.float32), design.astype(jnp.float32), preferred_element_type=jnp.float32)
    projection = jnp.dot(design.T.astype(jnp.float32), record.astype(jnp.float32), preferred_element_type=jnp.float32)
    coefficients = solve_fit(gram_matrix, projection)
    design_wide = design.astype(jnp.float32)

    def type_sums(event_row):
        chosen = (event_row[:, None] + lag_offsets[None, :]).astype(jnp.int32).reshape(-1)
        picked = jnp.take(record, chosen, axis=0).reshape(MEMBERS, LAGS, 2 * POINTS)
        raw_sums = jnp.sum(picked.astype(jnp.float32), axis=0)
        picked_design = jnp.take(design_wide, chosen, axis=0).reshape(MEMBERS, LAGS, 2 * HARMONICS + 1)
        counted_design = jnp.sum(picked_design, axis=0)
        return raw_sums - jnp.dot(counted_design, coefficients, precision=lax.Precision.HIGHEST)
    totals = lax.map(type_sums, events)
    maps = (totals / MEMBERS).reshape(TYPES, LAGS, 2, POINTS)
    map_mean = jnp.sum(maps, axis=3, keepdims=True) / POINTS
    return maps - map_mean
```

```python
import functools

import jax
import jax.numpy as jnp
from jax import lax
from jax.experimental import pallas as pl
from jax.experimental.pallas import tpu as pltpu
from jax.sharding import PartitionSpec as P

HARMONICS = 4
TERMS = 2 * HARMONICS + 1
TWO_PI = 6.283185307179586
PAD = 128
CHUNK = 256
NT = (((1,), (1,)), ((), ()))
TN = (((0,), (0,)), ((), ()))


def regressor_rows(calendar_day):
    phases = jnp.repeat(calendar_day, 2).astype(jnp.float32) * (TWO_PI / 365.25)
    rows = [jnp.ones_like(phases)]
    for harmonic in range(1, HARMONICS + 1):
        rows.append(jnp.cos(harmonic * phases))
        rows.append(jnp.sin(harmonic * phases))
    rows += [jnp.zeros_like(phases)] * (16 - TERMS)
    return jnp.stack(rows, axis=0).astype(jnp.bfloat16)


def prepare(days_ref, design_ref, weights_ref, normal_ref):
    members, types = days_ref.shape
    depth = design_ref.shape[1]
    shifts = (weights_ref.shape[0] - 32) // types
    places = lax.broadcasted_iota(jnp.int32, (members, depth + PAD), 1) - PAD
    for kind in range(types):
        hits = (days_ref[:, kind : kind + 1] == places).astype(jnp.float32)
        histogram = jnp.sum(hits, axis=0, keepdims=True)
        wide = jnp.broadcast_to(histogram, (shifts, depth + PAD))
        rolled = pltpu.roll(wide, 0, 1, stride=1, stride_axis=0)
        weights_ref[kind * shifts : (kind + 1) * shifts, :] = rolled[:, PAD:].astype(jnp.bfloat16)
    design = design_ref[...]
    odd = lax.broadcasted_iota(jnp.int32, design.shape, 1) % 2
    wide_design = design.astype(jnp.float32)
    weights_ref[types * shifts : types * shifts + 16, :] = jnp.where(odd == 0, wide_design, 0.0).astype(jnp.bfloat16)
    weights_ref[types * shifts + 16 :, :] = jnp.where(odd == 1, wide_design, 0.0).astype(jnp.bfloat16)
    normal_ref[...] = lax.dot_general(design, weights_ref[...], NT, preferred_element_type=jnp.float32)


def split3(value):
    high = value.astype(jnp.bfloat16)
    rest = value - high.astype(jnp.float32)
    middle = rest.astype(jnp.bfloat16)
    low = (rest - middle.astype(jnp.float32)).astype(jnp.bfloat16)
    return high, middle, low


def compose(
    tm, space, members, all_points,
    fields, weights_ref, normal_ref, out_ref,
    xs, normals, left, whole, owned, codes, scales, got_codes, got_scales, sums, got_sums,
    x_sems, n_send, n_recv, c_send, c_recv, s_send, s_recv, m_send, m_recv,
):
    rows = out_ref.shape[0]
    chunks = xs.shape[0]
    count_rows = weights_ref.shape[0] - 32
    me = lax.axis_index("tm")
    here = lax.axis_index("space")

    def load(c):
        return pltpu.make_async_copy(
            fields.at[:, :, pl.ds(pl.multiple_of(c * CHUNK, CHUNK), CHUNK)], xs.at[c], x_sems.at[c]
        )

    lax.fori_loop(0, chunks, lambda c, _: (load(c).start(), 0)[1], 0)

    barrier = pltpu.get_barrier_semaphore()
    for i in range(1, tm):
        pl.semaphore_signal(barrier, inc=1, device_id={"tm": lax.rem(me + i, tm)})
    for i in range(1, space):
        pl.semaphore_signal(barrier, inc=1, device_id={"space": lax.rem(here + i, space)})
    pl.semaphore_wait(barrier, tm + space - 2)

    def send_normal(i):
        return pltpu.make_async_remote_copy(
            normal_ref, normals.at[i - 1], n_send.at[i - 1], n_recv.at[i - 1], device_id={"tm": lax.rem(me + i, tm)}
        )

    def send_code(i, c):
        peer = {"tm": lax.rem(me + i, tm)}
        return (
            pltpu.make_async_remote_copy(
                codes.at[i - 1, c], got_codes.at[i - 1, c], c_send.at[i - 1, c], c_recv.at[i - 1, c], device_id=peer
            ),
            pltpu.make_async_remote_copy(
                scales.at[i - 1, c], got_scales.at[i - 1, c], s_send.at[i - 1, c], s_recv.at[i - 1, c], device_id=peer
            ),
        )

    def send_sums(i):
        return pltpu.make_async_remote_copy(
            sums, got_sums.at[i - 1], m_send.at[i - 1], m_recv.at[i - 1],
            device_id={"space": lax.rem(here + i, space)},
        )

    for i in range(1, tm):
        send_normal(i).start()
    system = normal_ref[...]
    for i in range(1, tm):
        send_normal(i).wait()
        system = system + normals[i - 1]
    lines = lax.broadcasted_iota(jnp.int32, system.shape, 0)
    for k in range(TERMS):
        pivot = system[k : k + 1, :] / system[k : k + 1, count_rows + k : count_rows + k + 1]
        system = jnp.where(lines == k, pivot, system - system[:, count_rows + k : count_rows + k + 1] * pivot)
    fit = system[:, :count_rows]
    fit = jnp.where(lax.broadcasted_iota(jnp.int32, fit.shape, 0) < TERMS, fit, 0.0)
    odd = lax.broadcasted_iota(jnp.int32, fit.shape, 1) % 2
    fit = jnp.concatenate([jnp.where(odd == 0, fit, 0.0), jnp.where(odd == 1, fit, 0.0)], axis=0)
    high, middle, low = split3(fit)
    left[...] = jnp.concatenate([high, high, high, middle, middle, low], axis=0)

    def step(c, _):
        load(c).wait()
        block = xs[c].reshape(weights_ref.shape[1], CHUNK)
        raw = jnp.dot(weights_ref[...], block, preferred_element_type=jnp.float32)
        p_high, p_middle, p_low = split3(raw[count_rows:])
        right = jnp.concatenate([p_high, p_middle, p_low, p_high, p_middle, p_high], axis=0)
        whole[...] = raw[:count_rows] - lax.dot_general(left[...], right, TN, preferred_element_type=jnp.float32)
        for i in range(1, tm):
            peer = lax.rem(me + i, tm)
            part = whole[pl.ds(pl.multiple_of(peer * rows, rows), rows), :]
            top = jnp.max(jnp.abs(part), axis=0, keepdims=True)
            factor = jnp.where(top > 0.0, 32767.0 / jnp.where(top > 0.0, top, 1.0), 0.0)
            codes[i - 1, c] = jnp.round(part * factor).astype(jnp.int32).astype(jnp.int16)
            scales[i - 1, c] = top * (1.0 / 32767.0)
            for copy in send_code(i, c):
                copy.start()
        owned[c] = whole[pl.ds(pl.multiple_of(me * rows, rows), rows), :]
        return 0

    lax.fori_loop(0, chunks, step, 0)

    ones = jnp.ones((8, CHUNK), jnp.bfloat16)

    def gather(c, total):
        value = owned[c]
        for i in range(1, tm):
            for copy in send_code(i, c):
                copy.wait()
            value = value + got_codes[i - 1, c].astype(jnp.int32).astype(jnp.float32) * got_scales[i - 1, c]
        value = value * (1.0 / members)
        owned[c] = value
        for piece in split3(value):
            total = total + lax.dot_general(ones, piece, NT, preferred_element_type=jnp.float32)
        return total

    sums[...] = lax.fori_loop(0, chunks, gather, jnp.zeros((8, rows), jnp.float32))
    for i in range(1, space):
        send_sums(i).start()
    total = sums[...]
    for i in range(1, space):
        send_sums(i).wait()
        total = total + got_sums[i - 1]
    mean = lax.dot_general(
        total * (1.0 / (8 * all_points)), jnp.ones((8, CHUNK), jnp.float32), TN,
        precision=lax.Precision.HIGHEST, preferred_element_type=jnp.float32,
    )

    def finish(c, _):
        out_ref[:, pl.ds(pl.multiple_of(c * CHUNK, CHUNK), CHUNK)] = owned[c] - mean
        return 0

    lax.fori_loop(0, chunks, finish, 0)


def shards(tm, space, fields, calendar_day, events, lag_offsets):
    types, members = events.shape
    lag_count = lag_offsets.shape[0]
    days, variables, points = fields.shape
    depth = variables * days
    count_rows = types * lag_count * variables
    rows = count_rows // tm
    chunks = points // CHUNK
    places = 2 * (events - lax.axis_index("tm") * days).T
    weights, normal = pl.pallas_call(
        prepare,
        out_shape=(
            jax.ShapeDtypeStruct((count_rows + 32, depth), jnp.bfloat16),
            jax.ShapeDtypeStruct((16, count_rows + 32), jnp.float32),
        ),
        in_specs=[pl.BlockSpec(memory_space=pltpu.VMEM)] * 2,
        out_specs=[pl.BlockSpec(memory_space=pltpu.VMEM)] * 2,
        compiler_params=pltpu.CompilerParams(vmem_limit_bytes=48 * 2**20),
        name="prepare",
    )(places, regressor_rows(calendar_day))
    pairs = (tm - 1, chunks)
    dma = pltpu.SemaphoreType.DMA
    result = pl.pallas_call(
        functools.partial(compose, tm, space, members, points * space),
        out_shape=jax.ShapeDtypeStruct((rows, points), jnp.float32),
        in_specs=[
            pl.BlockSpec(memory_space=pl.ANY),
            pl.BlockSpec(memory_space=pltpu.VMEM),
            pl.BlockSpec(memory_space=pltpu.VMEM),
        ],
        out_specs=pl.BlockSpec(memory_space=pltpu.VMEM),
        scratch_shapes=[
            pltpu.VMEM((chunks, days, variables, CHUNK), jnp.bfloat16),
            pltpu.VMEM((tm - 1, 16, count_rows + 32), jnp.float32),
            pltpu.VMEM((192, count_rows), jnp.bfloat16),
            pltpu.VMEM((count_rows, CHUNK), jnp.float32),
            pltpu.VMEM((chunks, rows, CHUNK), jnp.float32),
            pltpu.VMEM(pairs + (rows, CHUNK), jnp.int16),
            pltpu.VMEM(pairs + (1, CHUNK), jnp.float32),
            pltpu.VMEM(pairs + (rows, CHUNK), jnp.int16),
            pltpu.VMEM(pairs + (1, CHUNK), jnp.float32),
            pltpu.VMEM((8, rows), jnp.float32),
            pltpu.VMEM((space - 1, 8, rows), jnp.float32),
            dma((chunks,)),
            dma((tm - 1,)), dma((tm - 1,)),
            dma(pairs), dma(pairs), dma(pairs), dma(pairs),
            dma((space - 1,)), dma((space - 1,)),
        ],
        compiler_params=pltpu.CompilerParams(
            collective_id=0, has_side_effects=True, vmem_limit_bytes=60 * 2**20
        ),
        name="compose",
    )(fields, weights, normal)
    maps = result.reshape(types // tm, lag_count, variables, points)
    return jnp.take(maps, lag_offsets, axis=1)


def solution(mesh):
    return jax.shard_map(
        functools.partial(shards, mesh.shape["tm"], mesh.shape["space"]),
        mesh=mesh,
        in_specs=(P("tm", None, "space"), P("tm"), P(), P()),
        out_specs=P("tm", None, None, "space"),
        check_vma=False,
    )
```

```python
import functools

import jax
import jax.numpy as jnp
from jax import lax
from jax.experimental import pallas as pl
from jax.experimental.pallas import tpu as pltpu
from jax.sharding import PartitionSpec as P

HARMONICS = 4
TERMS = 2 * HARMONICS + 1
TWO_PI = 6.283185307179586
PAD = 128
CHUNK = 256
NT = (((1,), (1,)), ((), ()))
TN = (((0,), (0,)), ((), ()))


def regressor_rows(calendar_day):
    phases = jnp.repeat(calendar_day, 2).astype(jnp.float32) * (TWO_PI / 365.25)
    line = lax.iota(jnp.int32, 16)[:, None]
    angles = ((line + 1) // 2).astype(jnp.float32) * phases[None, :]
    rows = jnp.where(line % 2 == 1, jnp.cos(angles), jnp.sin(angles))
    rows = jnp.where(line == 0, 1.0, jnp.where(line < TERMS, rows, 0.0))
    return rows.astype(jnp.bfloat16)


def prepare(days_ref, design_ref, weights_ref, normal_ref):
    members, types = days_ref.shape
    depth = design_ref.shape[1]
    shifts = (weights_ref.shape[0] - 32) // types
    places = lax.broadcasted_iota(jnp.int32, (members, depth + PAD), 1) - PAD
    for kind in range(types):
        hits = (days_ref[:, kind : kind + 1] == places).astype(jnp.float32)
        histogram = jnp.sum(hits, axis=0, keepdims=True)
        wide = jnp.broadcast_to(histogram, (shifts, depth + PAD))
        rolled = pltpu.roll(wide, 0, 1, stride=1, stride_axis=0)
        weights_ref[kind * shifts : (kind + 1) * shifts, :] = rolled[:, PAD:].astype(jnp.bfloat16)
    design = design_ref[...]
    odd = lax.broadcasted_iota(jnp.int32, design.shape, 1) % 2
    wide_design = design.astype(jnp.float32)
    weights_ref[types * shifts : types * shifts + 16, :] = jnp.where(odd == 0, wide_design, 0.0).astype(jnp.bfloat16)
    weights_ref[types * shifts + 16 :, :] = jnp.where(odd == 1, wide_design, 0.0).astype(jnp.bfloat16)
    normal_ref[...] = lax.dot_general(design, weights_ref[...], NT, preferred_element_type=jnp.float32)


def split3(value):
    high = value.astype(jnp.bfloat16)
    rest = value - high.astype(jnp.float32)
    middle = rest.astype(jnp.bfloat16)
    low = (rest - middle.astype(jnp.float32)).astype(jnp.bfloat16)
    return high, middle, low


def encode(part):
    top = jnp.max(jnp.abs(part), axis=0, keepdims=True)
    factor = jnp.where(top > 0.0, 32767.0 / jnp.where(top > 0.0, top, 1.0), 0.0)
    return jnp.round(part * factor).astype(jnp.int32).astype(jnp.int16), top * (1.0 / 32767.0)


def decode(codes, scale):
    return codes.astype(jnp.int32).astype(jnp.float32) * scale


def flip(index, bits):
    bit = 1
    flipped = index
    while bit <= bits:
        if bits & bit:
            flipped = flipped + bit - 2 * bit * lax.rem(lax.div(index, bit), 2)
        bit *= 2
    return flipped


def compose(
    tm, space, members, all_points,
    fields, weights_hbm, normal_ref, out_ref, mean_ref,
    xs, weights_ref, normals, left, whole, parts, codes, scales, got_codes, got_scales, sums, got_sums,
    w_sem, x_sems, n_send, n_recv, c_send, c_recv, s_send, s_recv, m_send, m_recv,
):
    chunks, rows, _ = out_ref.shape
    count_rows = weights_ref.shape[0] - 32
    me = lax.axis_index("tm")
    here = lax.axis_index("space")
    stages = tm.bit_length() - 1

    def load(c):
        return pltpu.make_async_copy(
            fields.at[:, :, pl.ds(pl.multiple_of(c * CHUNK, CHUNK), CHUNK)], xs.at[c], x_sems.at[c]
        )

    load_weights = pltpu.make_async_copy(weights_hbm, weights_ref, w_sem)
    load_weights.start()
    lax.fori_loop(0, chunks, lambda c, _: (load(c).start(), 0)[1], 0)

    barrier = pltpu.get_barrier_semaphore()
    for i in range(1, tm):
        pl.semaphore_signal(barrier, inc=1, device_id={"tm": lax.rem(me + i, tm)})
    for i in range(1, space):
        pl.semaphore_signal(barrier, inc=1, device_id={"space": lax.rem(here + i, space)})
    pl.semaphore_wait(barrier, tm + space - 2)

    def send_normal(i):
        return pltpu.make_async_remote_copy(
            normal_ref, normals.at[i - 1], n_send.at[i - 1], n_recv.at[i - 1], device_id={"tm": lax.rem(me + i, tm)}
        )

    def send_code(apart, bit, c):
        peer = {"tm": flip(me, bit)}
        d = apart - 1
        return (
            pltpu.make_async_remote_copy(
                codes.at[d, c], got_codes.at[d, c], c_send.at[d, c], c_recv.at[d, c], device_id=peer
            ),
            pltpu.make_async_remote_copy(
                scales.at[d, c], got_scales.at[d, c], s_send.at[d, c], s_recv.at[d, c], device_id=peer
            ),
        )

    def send_sums(i):
        return pltpu.make_async_remote_copy(
            sums, got_sums.at[i - 1], m_send.at[i - 1], m_recv.at[i - 1],
            device_id={"space": lax.rem(here + i, space)},
        )

    for i in range(1, tm):
        send_normal(i).start()
    system = normal_ref[...]
    for i in range(1, tm):
        send_normal(i).wait()
        system = system + normals[i - 1]
    lines = lax.broadcasted_iota(jnp.int32, system.shape, 0)
    for k in range(TERMS):
        pivot = system[k : k + 1, :] / system[k : k + 1, count_rows + k : count_rows + k + 1]
        system = jnp.where(lines == k, pivot, system - system[:, count_rows + k : count_rows + k + 1] * pivot)
    fit = system[:, :count_rows]
    fit = jnp.where(lax.broadcasted_iota(jnp.int32, fit.shape, 0) < TERMS, fit, 0.0)
    odd = lax.broadcasted_iota(jnp.int32, fit.shape, 1) % 2
    fit = jnp.concatenate([jnp.where(odd == 0, fit, 0.0), jnp.where(odd == 1, fit, 0.0)], axis=0)
    high, middle, low = split3(fit)
    left[...] = jnp.concatenate([high, high, high, middle, middle, low], axis=0)
    load_weights.wait()

    def bits_of(turn):
        return [1 << ((turn + stage) % stages) for stage in range(stages)]

    def leaving(turn, stage):
        bits = bits_of(turn)
        return [
            apart for apart in range(1, tm)
            if apart & bits[stage] and not any(apart & bit for bit in bits[:stage])
        ]

    def each_chunk(body, start):
        def group(g, carry):
            for turn in range(stages):
                carry = body(g * stages + turn, turn, carry)
            return carry

        return lax.fori_loop(0, chunks // stages, group, start)

    def post(c, turn, stage):
        for apart in leaving(turn, stage):
            codes[apart - 1, c], scales[apart - 1, c] = encode(parts[apart, c])
            for copy in send_code(apart, bits_of(turn)[stage], c):
                copy.start()

    def collect(c, turn, stage):
        bit = bits_of(turn)[stage]
        for apart in leaving(turn, stage):
            for copy in send_code(apart, bit, c):
                copy.wait()
            parts[apart - bit, c] += decode(got_codes[apart - 1, c], got_scales[apart - 1, c])

    def compute(c, turn, carry):
        load(c).wait()
        block = xs[c].reshape(weights_ref.shape[1], CHUNK)
        raw = jnp.dot(weights_ref[...], block, preferred_element_type=jnp.float32)
        p_high, p_middle, p_low = split3(raw[count_rows:])
        right = jnp.concatenate([p_high, p_middle, p_low, p_high, p_middle, p_high], axis=0)
        whole[...] = raw[:count_rows] - lax.dot_general(left[...], right, TN, preferred_element_type=jnp.float32)
        for apart in range(tm):
            parts[apart, c] = whole[pl.ds(pl.multiple_of(flip(me, apart) * rows, rows), rows), :]
        post(c, turn, 0)
        return carry

    each_chunk(compute, 0)

    for stage in range(1, stages):
        def relay(c, turn, carry):
            collect(c, turn, stage - 1)
            post(c, turn, stage)
            return carry

        each_chunk(relay, 0)

    ones = jnp.ones((8, CHUNK), jnp.bfloat16)

    def gather(c, turn, total):
        collect(c, turn, stages - 1)
        value = parts[0, c] * (1.0 / members)
        out_ref[c] = value
        for piece in split3(value):
            total = total + lax.dot_general(ones, piece, NT, preferred_element_type=jnp.float32)
        return total

    sums[...] = each_chunk(gather, jnp.zeros((8, rows), jnp.float32))
    for i in range(1, space):
        send_sums(i).start()
    total = sums[...]
    for i in range(1, space):
        send_sums(i).wait()
        total = total + got_sums[i - 1]
    mean_ref[...] = lax.dot_general(
        total * (1.0 / (8 * all_points)), jnp.ones((8, CHUNK), jnp.float32), TN,
        precision=lax.Precision.HIGHEST, preferred_element_type=jnp.float32,
    )


def finish(lags_ref, values_ref, mean_ref, out_ref, natural):
    chunks = values_ref.shape[0]
    lag_count = out_ref.shape[1]
    mean = mean_ref[...]
    for c in range(chunks):
        centred = values_ref[c] - mean
        natural[:, :, c * CHUNK : (c + 1) * CHUNK] = centred.reshape(lag_count, 2, CHUNK)
    for lag in range(lag_count):
        out_ref[0, lag] = natural[lags_ref[lag]]


def shards(tm, space, fields, calendar_day, events, lag_offsets):
    types, members = events.shape
    lag_count = lag_offsets.shape[0]
    days, variables, points = fields.shape
    depth = variables * days
    count_rows = types * lag_count * variables
    rows = count_rows // tm
    chunks = points // CHUNK
    places = 2 * (events - lax.axis_index("tm") * days).T
    weights, normal = pl.pallas_call(
        prepare,
        out_shape=(
            jax.ShapeDtypeStruct((count_rows + 32, depth), jnp.bfloat16),
            jax.ShapeDtypeStruct((16, count_rows + 32), jnp.float32),
        ),
        in_specs=[pl.BlockSpec(memory_space=pltpu.VMEM)] * 2,
        out_specs=[pl.BlockSpec(memory_space=pltpu.VMEM)] * 2,
        compiler_params=pltpu.CompilerParams(vmem_limit_bytes=48 * 2**20),
        name="prepare",
    )(places, regressor_rows(calendar_day))
    pairs = (tm - 1, chunks)
    dma = pltpu.SemaphoreType.DMA
    values, mean = pl.pallas_call(
        functools.partial(compose, tm, space, members, points * space),
        out_shape=(
            jax.ShapeDtypeStruct((chunks, rows, CHUNK), jnp.float32),
            jax.ShapeDtypeStruct((rows, CHUNK), jnp.float32),
        ),
        in_specs=[
            pl.BlockSpec(memory_space=pl.ANY),
            pl.BlockSpec(memory_space=pl.ANY),
            pl.BlockSpec(memory_space=pltpu.VMEM),
        ],
        out_specs=[pl.BlockSpec(memory_space=pltpu.VMEM)] * 2,
        scratch_shapes=[
            pltpu.VMEM((chunks, days, variables, CHUNK), jnp.bfloat16),
            pltpu.VMEM((count_rows + 32, depth), jnp.bfloat16),
            pltpu.VMEM((tm - 1, 16, count_rows + 32), jnp.float32),
            pltpu.VMEM((192, count_rows), jnp.bfloat16),
            pltpu.VMEM((count_rows, CHUNK), jnp.float32),
            pltpu.VMEM((tm, chunks, rows, CHUNK), jnp.float32),
            pltpu.VMEM(pairs + (rows, CHUNK), jnp.int16),
            pltpu.VMEM(pairs + (1, CHUNK), jnp.float32),
            pltpu.VMEM(pairs + (rows, CHUNK), jnp.int16),
            pltpu.VMEM(pairs + (1, CHUNK), jnp.float32),
            pltpu.VMEM((8, rows), jnp.float32),
            pltpu.VMEM((space - 1, 8, rows), jnp.float32),
            dma, dma((chunks,)),
            dma((tm - 1,)), dma((tm - 1,)),
            dma(pairs), dma(pairs), dma(pairs), dma(pairs),
            dma((space - 1,)), dma((space - 1,)),
        ],
        compiler_params=pltpu.CompilerParams(
            collective_id=0, has_side_effects=True, vmem_limit_bytes=60 * 2**20
        ),
        name="compose",
    )(fields, weights, normal)
    shifts = lag_count * variables
    return pl.pallas_call(
        finish,
        grid=(types // tm,),
        out_shape=jax.ShapeDtypeStruct((types // tm, lag_count, variables, points), jnp.float32),
        in_specs=[
            pl.BlockSpec(memory_space=pltpu.SMEM),
            pl.BlockSpec((chunks, shifts, CHUNK), lambda kind: (0, kind, 0)),
            pl.BlockSpec((shifts, CHUNK), lambda kind: (kind, 0)),
        ],
        out_specs=pl.BlockSpec((1, lag_count, variables, points), lambda kind: (kind, 0, 0, 0)),
        scratch_shapes=[pltpu.VMEM((lag_count, variables, points), jnp.float32)],
        name="finish",
    )(lag_offsets, values, mean)


def solution(mesh):
    return jax.shard_map(
        functools.partial(shards, mesh.shape["tm"], mesh.shape["space"]),
        mesh=mesh,
        in_specs=(P("tm", None, "space"), P("tm"), P(), P()),
        out_specs=P("tm", None, None, "space"),
        check_vma=False,
    )
```

```python
import functools

import jax
import jax.numpy as jnp
from jax import lax
from jax.experimental import pallas as pl
from jax.experimental.pallas import tpu as pltpu
from jax.sharding import PartitionSpec as P

HARMONICS = 4
TERMS = 2 * HARMONICS + 1
TWO_PI = 6.283185307179586
PAD = 128
CHUNK = 256
NT = (((1,), (1,)), ((), ()))
TN = (((0,), (0,)), ((), ()))


def regressor_rows(calendar_day):
    phases = jnp.repeat(calendar_day, 2).astype(jnp.float32) * (TWO_PI / 365.25)
    line = lax.iota(jnp.int32, 16)[:, None]
    angles = ((line + 1) // 2).astype(jnp.float32) * phases[None, :]
    rows = jnp.where(line % 2 == 1, jnp.cos(angles), jnp.sin(angles))
    rows = jnp.where(line == 0, 1.0, jnp.where(line < TERMS, rows, 0.0))
    return rows.astype(jnp.bfloat16)


def prepare(days_ref, design_ref, weights_ref, normal_ref):
    members, types = days_ref.shape
    depth = design_ref.shape[1]
    shifts = (weights_ref.shape[0] - 32) // types
    places = lax.broadcasted_iota(jnp.int32, (members, depth + PAD), 1) - PAD
    for kind in range(types):
        hits = (days_ref[:, kind : kind + 1] == places).astype(jnp.float32)
        histogram = jnp.sum(hits, axis=0, keepdims=True)
        wide = jnp.broadcast_to(histogram, (shifts, depth + PAD))
        rolled = pltpu.roll(wide, 0, 1, stride=1, stride_axis=0)
        weights_ref[kind * shifts : (kind + 1) * shifts, :] = rolled[:, PAD:].astype(jnp.bfloat16)
    design = design_ref[...]
    odd = lax.broadcasted_iota(jnp.int32, design.shape, 1) % 2
    wide_design = design.astype(jnp.float32)
    weights_ref[types * shifts : types * shifts + 16, :] = jnp.where(odd == 0, wide_design, 0.0).astype(jnp.bfloat16)
    weights_ref[types * shifts + 16 :, :] = jnp.where(odd == 1, wide_design, 0.0).astype(jnp.bfloat16)
    normal_ref[...] = lax.dot_general(design, weights_ref[...], NT, preferred_element_type=jnp.float32)


def split3(value):
    high = value.astype(jnp.bfloat16)
    rest = value - high.astype(jnp.float32)
    middle = rest.astype(jnp.bfloat16)
    low = (rest - middle.astype(jnp.float32)).astype(jnp.bfloat16)
    return high, middle, low


def encode(part):
    top = jnp.max(jnp.abs(part), axis=0, keepdims=True)
    factor = jnp.where(top > 0.0, 32767.0 / jnp.where(top > 0.0, top, 1.0), 0.0)
    return jnp.round(part * factor).astype(jnp.int32).astype(jnp.int16), top * (1.0 / 32767.0)


def decode(codes, scale):
    return codes.astype(jnp.int32).astype(jnp.float32) * scale


def flip(index, bits):
    bit = 1
    flipped = index
    while bit <= bits:
        if bits & bit:
            flipped = flipped + bit - 2 * bit * lax.rem(lax.div(index, bit), 2)
        bit *= 2
    return flipped


def compose(
    tm, space, members, all_points,
    fields, weights_hbm, normal_ref, out_ref, mean_ref,
    xs, weights_ref, normals, left, whole, parts, codes, scales, got_codes, got_scales, sums, got_sums,
    w_sem, x_sems, n_send, n_recv, c_send, c_recv, s_send, s_recv, m_send, m_recv,
):
    chunks, rows, _ = out_ref.shape
    count_rows = weights_ref.shape[0] - 32
    me = lax.axis_index("tm")
    here = lax.axis_index("space")
    stages = tm.bit_length() - 1

    def load(c):
        return pltpu.make_async_copy(
            fields.at[:, :, pl.ds(pl.multiple_of(c * CHUNK, CHUNK), CHUNK)], xs.at[c], x_sems.at[c]
        )

    load_weights = pltpu.make_async_copy(weights_hbm, weights_ref, w_sem)
    load_weights.start()
    lax.fori_loop(0, chunks, lambda c, _: (load(c).start(), 0)[1], 0)

    barrier = pltpu.get_barrier_semaphore()
    for i in range(1, tm):
        pl.semaphore_signal(barrier, inc=1, device_id={"tm": lax.rem(me + i, tm)})
    for i in range(1, space):
        pl.semaphore_signal(barrier, inc=1, device_id={"space": lax.rem(here + i, space)})
    pl.semaphore_wait(barrier, tm + space - 2)

    def send_normal(i):
        return pltpu.make_async_remote_copy(
            normal_ref, normals.at[i - 1], n_send.at[i - 1], n_recv.at[i - 1], device_id={"tm": lax.rem(me + i, tm)}
        )

    def send_code(apart, bit, c):
        peer = {"tm": flip(me, bit)}
        d = apart - 1
        return (
            pltpu.make_async_remote_copy(
                codes.at[d, c], got_codes.at[d, c], c_send.at[d, c], c_recv.at[d, c], device_id=peer
            ),
            pltpu.make_async_remote_copy(
                scales.at[d, c], got_scales.at[d, c], s_send.at[d, c], s_recv.at[d, c], device_id=peer
            ),
        )

    def send_sums(i):
        return pltpu.make_async_remote_copy(
            sums, got_sums.at[i - 1], m_send.at[i - 1], m_recv.at[i - 1],
            device_id={"space": lax.rem(here + i, space)},
        )

    for i in range(1, tm):
        send_normal(i).start()
    system = normal_ref[...]
    for i in range(1, tm):
        send_normal(i).wait()
        system = system + normals[i - 1]
    lines = lax.broadcasted_iota(jnp.int32, system.shape, 0)
    for k in range(TERMS):
        pivot = system[k : k + 1, :] / system[k : k + 1, count_rows + k : count_rows + k + 1]
        system = jnp.where(lines == k, pivot, system - system[:, count_rows + k : count_rows + k + 1] * pivot)
    fit = system[:, :count_rows]
    fit = jnp.where(lax.broadcasted_iota(jnp.int32, fit.shape, 0) < TERMS, fit, 0.0)
    odd = lax.broadcasted_iota(jnp.int32, fit.shape, 1) % 2
    fit = jnp.concatenate([jnp.where(odd == 0, fit, 0.0), jnp.where(odd == 1, fit, 0.0)], axis=0)
    high, middle, low = split3(fit)
    left[...] = jnp.concatenate([high, high, high, middle, middle, low], axis=0)
    load_weights.wait()

    def bits_of(turn):
        return [1 << ((turn + stage) % stages) for stage in range(stages)]

    def leaving(turn, stage):
        bits = bits_of(turn)
        return [
            apart for apart in range(1, tm)
            if apart & bits[stage] and not any(apart & bit for bit in bits[:stage])
        ]

    def each_chunk(body, start):
        def group(g, carry):
            for turn in range(stages):
                carry = body(g * stages + turn, turn, carry)
            return carry

        return lax.fori_loop(0, chunks // stages, group, start)

    def post(c, turn, stage):
        for apart in leaving(turn, stage):
            codes[apart - 1, c], scales[apart - 1, c] = encode(parts[apart, c])
            for copy in send_code(apart, bits_of(turn)[stage], c):
                copy.start()

    def collect(c, turn, stage):
        bit = bits_of(turn)[stage]
        for apart in leaving(turn, stage):
            for copy in send_code(apart, bit, c):
                copy.wait()
            parts[apart - bit, c] += decode(got_codes[apart - 1, c], got_scales[apart - 1, c])

    def compute(c, turn, carry):
        load(c).wait()
        block = xs[c].reshape(weights_ref.shape[1], CHUNK)
        raw = jnp.dot(weights_ref[...], block, preferred_element_type=jnp.float32)
        p_high, p_middle, p_low = split3(raw[count_rows:])
        right = jnp.concatenate([p_high, p_middle, p_low, p_high, p_middle, p_high], axis=0)
        whole[...] = raw[:count_rows] - lax.dot_general(left[...], right, TN, preferred_element_type=jnp.float32)
        for apart in range(tm):
            parts[apart, c] = whole[pl.ds(pl.multiple_of(flip(me, apart) * rows, rows), rows), :]
        post(c, turn, 0)
        return carry

    each_chunk(compute, 0)

    for stage in range(1, stages):
        def relay(c, turn, carry):
            collect(c, turn, stage - 1)
            post(c, turn, stage)
            return carry

        each_chunk(relay, 0)

    ones = jnp.ones((8, CHUNK), jnp.bfloat16)

    def gather(c, turn, total):
        collect(c, turn, stages - 1)
        value = parts[0, c] * (1.0 / members)
        out_ref[c] = value
        for piece in split3(value):
            total = total + lax.dot_general(ones, piece, NT, preferred_element_type=jnp.float32)
        return total

    sums[...] = each_chunk(gather, jnp.zeros((8, rows), jnp.float32))
    for i in range(1, space):
        send_sums(i).start()
    total = sums[...]
    for i in range(1, space):
        send_sums(i).wait()
        total = total + got_sums[i - 1]
    mean_ref[...] = lax.dot_general(
        total * (1.0 / (8 * all_points)), jnp.ones((8, CHUNK), jnp.float32), TN,
        precision=lax.Precision.HIGHEST, preferred_element_type=jnp.float32,
    )


def finish(lags_ref, values_ref, mean_ref, out_ref, natural):
    chunks = values_ref.shape[0]
    lag_count = out_ref.shape[1]
    mean = mean_ref[...]
    for c in range(chunks):
        centred = values_ref[c] - mean
        natural[:, :, c * CHUNK : (c + 1) * CHUNK] = centred.reshape(lag_count, 2, CHUNK)
    for lag in range(lag_count):
        out_ref[0, lag] = natural[lags_ref[lag]]


def shards(tm, space, fields, calendar_day, events, lag_offsets):
    types, members = events.shape
    lag_count = lag_offsets.shape[0]
    days, variables, points = fields.shape
    depth = variables * days
    count_rows = types * lag_count * variables
    rows = count_rows // tm
    chunks = points // CHUNK
    places = 2 * (events - lax.axis_index("tm") * days).T
    weights, normal = pl.pallas_call(
        prepare,
        out_shape=(
            jax.ShapeDtypeStruct((count_rows + 32, depth), jnp.bfloat16),
            jax.ShapeDtypeStruct((16, count_rows + 32), jnp.float32),
        ),
        in_specs=[pl.BlockSpec(memory_space=pltpu.VMEM)] * 2,
        out_specs=[pl.BlockSpec(memory_space=pltpu.VMEM)] * 2,
        compiler_params=pltpu.CompilerParams(vmem_limit_bytes=48 * 2**20),
        name="prepare",
    )(places, regressor_rows(calendar_day))
    pairs = (tm - 1, chunks)
    dma = pltpu.SemaphoreType.DMA
    values, mean = pl.pallas_call(
        functools.partial(compose, tm, space, members, points * space),
        out_shape=(
            jax.ShapeDtypeStruct((chunks, rows, CHUNK), jnp.float32),
            jax.ShapeDtypeStruct((rows, CHUNK), jnp.float32),
        ),
        in_specs=[
            pl.BlockSpec(memory_space=pl.ANY),
            pl.BlockSpec(memory_space=pl.ANY),
            pl.BlockSpec(memory_space=pltpu.VMEM),
        ],
        out_specs=[pl.BlockSpec(memory_space=pltpu.VMEM)] * 2,
        scratch_shapes=[
            pltpu.VMEM((chunks, days, variables, CHUNK), jnp.bfloat16),
            pltpu.VMEM((count_rows + 32, depth), jnp.bfloat16),
            pltpu.VMEM((tm - 1, 16, count_rows + 32), jnp.float32),
            pltpu.VMEM((192, count_rows), jnp.bfloat16),
            pltpu.VMEM((count_rows, CHUNK), jnp.float32),
            pltpu.VMEM((tm, chunks, rows, CHUNK), jnp.float32),
            pltpu.VMEM(pairs + (rows, CHUNK), jnp.int16),
            pltpu.VMEM(pairs + (1, CHUNK), jnp.float32),
            pltpu.VMEM(pairs + (rows, CHUNK), jnp.int16),
            pltpu.VMEM(pairs + (1, CHUNK), jnp.float32),
            pltpu.VMEM((8, rows), jnp.float32),
            pltpu.VMEM((space - 1, 8, rows), jnp.float32),
            dma, dma((chunks,)),
            dma((tm - 1,)), dma((tm - 1,)),
            dma(pairs), dma(pairs), dma(pairs), dma(pairs),
            dma((space - 1,)), dma((space - 1,)),
        ],
        compiler_params=pltpu.CompilerParams(
            collective_id=0, has_side_effects=True, vmem_limit_bytes=48 * 2**20
        ),
        name="compose",
    )(fields, weights, normal)
    shifts = lag_count * variables
    return pl.pallas_call(
        finish,
        grid=(types // tm,),
        out_shape=jax.ShapeDtypeStruct((types // tm, lag_count, variables, points), jnp.float32),
        in_specs=[
            pl.BlockSpec(memory_space=pltpu.SMEM),
            pl.BlockSpec((chunks, shifts, CHUNK), lambda kind: (0, kind, 0)),
            pl.BlockSpec((shifts, CHUNK), lambda kind: (kind, 0)),
        ],
        out_specs=pl.BlockSpec((1, lag_count, variables, points), lambda kind: (kind, 0, 0, 0)),
        scratch_shapes=[pltpu.VMEM((lag_count, variables, points), jnp.float32)],
        compiler_params=pltpu.CompilerParams(vmem_limit_bytes=40 * 2**20),
        name="finish",
    )(lag_offsets, values, mean)


def solution(mesh):
    return jax.shard_map(
        functools.partial(shards, mesh.shape["tm"], mesh.shape["space"]),
        mesh=mesh,
        in_specs=(P("tm", None, "space"), P("tm"), P(), P()),
        out_specs=P("tm", None, None, "space"),
        check_vma=False,
    )
```
